512 devices in a mesh: grp: 64 (over z, x_lo, core), tp: 8 (over x_hi, y).
Axes of the slice: x: 4 (x_hi: 2, x_lo: 2; x = x_hi * 2 + x_lo), y: 4, z: 16, core: 2. Of those that a mesh axis runs over, the one named last changes fastest.
Arguments:
- memory_rows: bfloat16 [65536, 4096], P('grp', 'tp'), may hold values from -24 to 24, as said below
- norm_gain: float32 [4096], replicated, may hold values from 0.25 to 1.75
- key_weight: bfloat16 [4096, 4096], P(None, 'tp'), may hold values from -0.09375 to 0.09375
- owner_table: int32 [8192], replicated, may hold values from 0 to 8191, as said below
Outputs:
- placed_keys: bfloat16 [65536, 4096], P('grp', 'tp')
The draws below stay inside these ranges and needn't reach their ends.
Inputs may be any that keep to these rules, and one draw needn't show every extreme that they name: A permutation of the 8192 block numbers. Block b of the input goes to block position owner_table[b], which lies in group owner_table[b] // 128. The 128 blocks of one group go to all 64 groups, exactly 2 blocks to each of them. `memory_rows`: rows have offsets and scales of their own, and features a common pattern.
All inputs are finite; a program needn't handle non-finite values.
Results may differ from the reference program's by a relative error of at most 0.0049.
Values may be sent and summed in bfloat16 or wider, within the bound.
A program may use at most 64 MiB of HBM per device.

```python
import jax
import jax.numpy as jnp
from jax import lax

D = 4096
BLK_ROWS = 8
BLK_DEV = 128
ROWS = 65536
NB = 8192


def draw_memory_rows(key, part):
    key_off, key_scale, key_noise, key_pattern = jax.random.split(key, 4)
    offsets = jax.random.uniform(key_off, (ROWS, 1), jnp.float32, -1.5, 1.5)
    pattern = jnp.clip(jax.random.normal(key_pattern, (1, D), jnp.float32), -3.0, 3.0)
    scales = jnp.exp(jax.random.uniform(key_scale, (ROWS, 1), jnp.float32, jnp.log(0.5), jnp.log(3.0)))
    noise = jnp.clip(jax.random.normal(key_noise, (ROWS, D), jnp.float32), -4.0, 4.0)
    values = offsets + scales * (noise + 0.7 * pattern)
    return jnp.clip(values, -24.0, 24.0).astype(jnp.bfloat16)


def draw_owner_table(key, part):
    groups = NB // BLK_DEV
    per_pair = BLK_DEV // groups
    key_tau, key_offs, key_cols, key_slots = jax.random.split(key, 4)
    shuffle = jax.random.permutation(key_tau, groups).astype(jnp.int32)
    offsets = jax.random.permutation(key_offs, groups).astype(jnp.int32)
    column_keys = jax.random.split(key_cols, groups)
    column_perm = jax.vmap(lambda one_key: jax.random.permutation(one_key, BLK_DEV))(column_keys).astype(jnp.int32)
    sources = jnp.arange(groups, dtype=jnp.int32)[:, None]
    target = shuffle[(sources + offsets[column_perm % groups]) % groups]
    arrival = sources * per_pair + column_perm // groups
    slot_keys = jax.random.split(key_slots, groups)
    slot_perm = jax.vmap(lambda one_key: jax.random.permutation(one_key, BLK_DEV))(slot_keys).astype(jnp.int32)
    slots = slot_perm[target, arrival]
    return (target * BLK_DEV + slots).reshape(-1).astype(jnp.int32)


def level_of(own_key, extent, cuts, low, high):
    def one(axis_at, blocks):
        draws = jax.random.uniform(jax.random.fold_in(jax.random.fold_in(own_key, 6), axis_at), (blocks,), jnp.float32, low / len(cuts), high / len(cuts))
        return jnp.repeat(jnp.exp(draws), extent[axis_at] // blocks).reshape((-1,) + (1,) * (len(extent) - axis_at - 1))

    factor_of = one(*cuts[0])
    for cut in cuts[1:]:
        factor_of = factor_of * one(*cut)
    return factor_of


def normal_values(rng, dims, width, reach, cuts=(), kind=jnp.bfloat16):
    values = jax.random.normal(rng, dims, jnp.float32) * width
    if len(cuts) > 0:
        values = level_of(rng, dims, cuts, -0.22, 0.18) * values
    return jnp.clip(values, min=-reach, max=reach).astype(kind)


def setup_inputs(seed: int = 0) -> dict:
    arg_keys = jax.random.split(jax.random.key(seed), 5)
    memory_rows = draw_memory_rows(jax.random.fold_in(arg_keys[4], 71), 0)
    norm_gain = jnp.clip(1.0 + 0.15 * jax.random.normal(arg_keys[1], (D,), jnp.float32), 0.25, 1.75)
    key_weight = normal_values(arg_keys[2], (D, D), D ** -0.5, 0.09375, ((1, 8),))
    owner_table = draw_owner_table(jax.random.fold_in(arg_keys[4], 71), 0)
    return dict(memory_rows=memory_rows, norm_gain=norm_gain, key_weight=key_weight, owner_table=owner_table)


EPS = 1e-05

def reference(memory_rows, norm_gain, key_weight, owner_table):
    values = memory_rows.astype(jnp.float32)
    row_sum = lax.optimization_barrier(jnp.sum(values, axis=1, keepdims=True))
    row_sq = lax.optimization_barrier(jnp.sum(values * values, axis=1, keepdims=True))
    row_mean = row_sum / D
    row_var = row_sq / D - row_mean * row_mean
    normed = ((values - row_mean) * lax.rsqrt(row_var + EPS) * norm_gain[None, :]).astype(jnp.bfloat16)
    keys = jnp.dot(normed, key_weight, preferred_element_type=jnp.float32).astype(jnp.bfloat16)
    blocks = keys.reshape(NB, BLK_ROWS, D)
    placed = jnp.zeros_like(blocks).at[owner_table.astype(jnp.int32)].set(blocks)
    return placed.reshape(ROWS, D)
```

```python
import functools

import jax
import jax.numpy as jnp
from jax import lax
from jax.experimental import pallas as pl
from jax.experimental.pallas import tpu as pltpu
from jax.sharding import PartitionSpec as P

BLK_ROWS = 8
EPS = 1e-05
MESH = pl.DeviceIdType.MESH

CPC = 2
FIRST = 5
BURST = 3


def class_shift(q, depth):
    return lax.rem(((q + 1) // 2) * (2 * lax.rem(q, 2) - 1) + depth, depth)


def tables(owner_table, depth):
    g = lax.axis_index("grp")
    z, xl, co = g // 4, (g // 2) % 2, g % 2
    blocks = 8 * depth
    groups = 4 * depth
    table = owner_table.reshape(groups, blocks)
    target = table // blocks
    own = lax.dynamic_slice_in_dim(target, g, 1, axis=0)[0]
    ids = jnp.arange(blocks, dtype=jnp.int32)
    rank = jnp.sum(
        ((own[None, :] == own[:, None]) & (ids[None, :] < ids[:, None])).astype(jnp.int32), axis=1
    )
    r = ids % 2
    k = (ids // 2) % CPC
    m = (ids // (2 * CPC)) % 4
    c = ids // (8 * CPC)
    q = c * CPC + k
    dz = ((q + 1) // 2) * (2 * (q % 2) - 1)
    dest = ((z + dz + depth) % depth) * 4 + m
    hit = (own[None, :] == dest[:, None]) & (rank[None, :] == r[:, None])
    order = jnp.sum(jnp.where(hit, ids[None, :], 0), axis=1)

    mine = target == g
    slot = table % blocks
    column = jnp.where(mine, ids[None, :], blocks)
    first = jnp.min(column, axis=1, keepdims=True)
    slot_first = jnp.sum(jnp.where(ids[None, :] == first, slot, 0), axis=1)
    slot_both = jnp.sum(jnp.where(mine, slot, 0), axis=1)
    slots = jnp.concatenate([slot_first, slot_both - slot_first])
    src = jnp.arange(2 * groups, dtype=jnp.int32) % groups
    which = jnp.arange(2 * groups, dtype=jnp.int32) // groups
    back = (z - src // 4 + depth) % depth
    q = jnp.where(back <= depth // 2, jnp.maximum(2 * back - 1, 0), 2 * (depth - back))
    dl = ((src // 2) % 2 + xl) % 2
    dc = (src % 2 + co) % 2
    where = (((q // CPC) * 4 + dl * 2 + dc) * CPC + q % CPC) * 2 + which
    place = jnp.sum(jnp.where(slots[None, :] == ids[:, None], where[None, :], 0), axis=1)
    return order, place


def flip(bit, by):
    return 1 - bit if by else bit


def refresh_kernel(
    depth,
    order,
    x_hbm,
    gain,
    w_hbm,
    found,
    xin,
    sorted_rows,
    gat,
    w_own,
    w_far,
    stats,
    part,
    arrived,
    load_sem,
    w_load_sem,
    z_send,
    z_recv,
    y_send,
    y_recv,
    r_send,
    r_recv,
    s_send,
    s_recv,
    x_send,
    x_recv,
    w_send,
    w_recv,
    d_send,
    d_recv,
):
    g, t = lax.axis_index("grp"), lax.axis_index("tp")
    z, xl, co = g // 4, lax.rem(g // 2, 2), lax.rem(g, 2)
    xh, y = t // 4, lax.rem(t, 4)
    chunks = depth // CPC
    dl_width = x_hbm.shape[-1]
    features = 8 * dl_width
    half_rows = 4 * dl_width
    rows_c = 64 * CPC

    def device(zz, xxl, cc, xxh, yy):
        return {"grp": zz * 4 + xxl * 2 + cc, "tp": xxh * 4 + yy}

    load = pltpu.make_async_copy(x_hbm, xin, load_sem)
    load.start()
    w_start = pl.multiple_of(xh * half_rows, half_rows)
    load_w = pltpu.make_async_copy(w_hbm.at[pl.ds(w_start, half_rows)], w_own, w_load_sem)
    load_w.start()

    barrier = pltpu.get_barrier_semaphore()
    partners = 0
    for step in range(1, depth):
        pl.semaphore_signal(
            barrier, inc=1, device_id=device(lax.rem(z + step, depth), xl, co, xh, y), device_id_type=MESH
        )
        partners += 1
    for step in range(1, 8):
        pl.semaphore_signal(
            barrier, inc=1, device_id={"grp": g, "tp": lax.rem(t + step, 8)}, device_id_type=MESH
        )
        partners += 1
    for j in range(1, 8):
        if j == 4:
            continue
        pl.semaphore_signal(
            barrier,
            inc=1,
            device_id=device(z, flip(xl, (j // 2) % 2), flip(co, j % 2), flip(xh, j // 4), y),
            device_id_type=MESH,
        )
        partners += 1

    load.wait()

    def sort_step(s, carry):
        cc = s // (8 * CPC)
        mm = lax.rem(s // (2 * CPC), 4)
        kk = lax.rem(s // 2, CPC)
        sorted_rows[cc, mm, kk, lax.rem(s, 2)] = xin[order[s]]
        return carry

    lax.fori_loop(0, 8 * depth, sort_step, 0, unroll=8)
    gat[y, 0, :, 0] = sorted_rows[0, :, 0]

    pl.semaphore_wait(barrier, partners)

    def z_copy(q):
        cc, kk = q // CPC, lax.rem(q, CPC)
        return pltpu.make_async_remote_copy(
            src_ref=sorted_rows.at[cc, :, kk],
            dst_ref=gat.at[y, cc, :, kk],
            send_sem=z_send.at[q],
            recv_sem=z_recv.at[q],
            device_id=device(lax.rem(z + class_shift(q, depth), depth), xl, co, xh, y),
            device_id_type=MESH,
        )

    def z_start(q, carry):
        z_copy(q).start()
        return carry

    lax.fori_loop(1, depth, z_start, 0)

    w_rows = half_rows // 2
    w_at = pl.multiple_of(co * w_rows, w_rows)
    w_copy = pltpu.make_async_remote_copy(
        src_ref=w_hbm.at[pl.ds(pl.multiple_of((1 - xh) * half_rows + w_at, w_rows), w_rows)],
        dst_ref=w_far.at[pl.ds(w_at, w_rows)],
        send_sem=w_send,
        recv_sem=w_recv,
        device_id=device(z, 1 - xl, co, 1 - xh, y),
        device_id_type=MESH,
    )
    w_copy.start()
    w_share = pltpu.make_async_remote_copy(
        src_ref=w_far.at[pl.ds(w_at, w_rows)],
        dst_ref=w_far.at[pl.ds(w_at, w_rows)],
        send_sem=d_send,
        recv_sem=d_recv,
        device_id=device(z, xl, 1 - co, xh, y),
        device_id_type=MESH,
    )

    left, right = lax.rem(y + 3, 4), lax.rem(y + 1, 4)

    def y_copy(side, c):
        return pltpu.make_async_remote_copy(
            src_ref=gat.at[y, c],
            dst_ref=gat.at[y, c],
            send_sem=y_send.at[side, c],
            recv_sem=y_recv.at[side, c],
            device_id=device(z, xl, co, xh, right if side == 0 else left),
            device_id_type=MESH,
        )

    def relay_copy(side, c):
        span = pl.ds(0, 2) if side == 0 else pl.ds(2, 2)
        piece = left if side == 0 else right
        return pltpu.make_async_remote_copy(
            src_ref=gat.at[piece, c, span],
            dst_ref=gat.at[piece, c, span],
            send_sem=r_send.at[side, c],
            recv_sem=r_recv.at[side, c],
            device_id=device(z, xl, co, xh, right if side == 0 else left),
            device_id_type=MESH,
        )

    def stats_copy(c, step):
        return pltpu.make_async_remote_copy(
            src_ref=stats.at[c, 0],
            dst_ref=stats.at[c, step],
            send_sem=s_send.at[c],
            recv_sem=s_recv.at[c],
            device_id={"grp": g, "tp": lax.rem(t + step, 8)},
            device_id_type=MESH,
        )

    def x_copy(c, j):
        dh, dl, dc = j // 4, (j // 2) % 2, j % 2
        to_l, to_c = flip(xl, dl), flip(co, dc)
        return pltpu.make_async_remote_copy(
            src_ref=part.at[c, dh, to_l * 2 + to_c],
            dst_ref=arrived.at[c, j],
            send_sem=x_send.at[c],
            recv_sem=x_recv.at[c],
            device_id=device(z, to_l, to_c, flip(xh, dh), y),
            device_id_type=MESH,
        )

    def take(c):
        for kk in range(CPC):
            q = c * CPC + kk
            if kk == 0:

                @pl.when(c > 0)
                def _():
                    z_copy(q).wait_recv()

            else:
                z_copy(q).wait_recv()
        y_copy(0, c).start()
        y_copy(1, c).start()
        v = gat[y, c].astype(jnp.float32).reshape(rows_c, dl_width)
        row_sum = jnp.sum(v, axis=1, keepdims=True)
        row_sq = jnp.sum(v * v, axis=1, keepdims=True)
        lane = lax.broadcasted_iota(jnp.int32, (rows_c, 128), 1)
        both = jnp.where(lane == 0, row_sum, jnp.where(lane == 1, row_sq, 0.0))
        stats[c, 0, :, pl.ds(0, rows_c)] = both.T[0:8, :]
        for step in range(1, 8):
            stats_copy(c, step).start()

    def relay(c):
        y_copy(0, c).wait_recv()
        relay_copy(0, c).start()
        y_copy(1, c).wait_recv()
        relay_copy(1, c).start()

    def multiply(c):
        relay_copy(0, c).wait_recv()
        relay_copy(1, c).wait_recv()
        all_stats = stats.at[c, pl.ds(1, 7)]
        pltpu.make_async_copy(all_stats, all_stats, s_recv.at[c]).wait()
        total = jnp.sum(stats[c], axis=0)[:, 0:rows_c]
        mean = total[0:1] / features
        var = total[1:2] / features - mean * mean
        rstd = lax.rsqrt(var + EPS)
        sub = lax.broadcasted_iota(jnp.int32, (128, rows_c), 0)
        columns = jnp.where(sub == 0, mean, rstd).T
        mean_c, rstd_c = columns[:, 0:1], columns[:, 1:2]
        near = jnp.zeros((rows_c, dl_width), jnp.float32)
        far = jnp.zeros((rows_c, dl_width), jnp.float32)
        for yy in range(4):
            v = gat[yy, c].astype(jnp.float32).reshape(rows_c, dl_width)
            scale = gain[0:1, pl.ds(pl.multiple_of(w_start + yy * dl_width, dl_width), dl_width)]
            normed = ((v - mean_c) * rstd_c * scale).astype(jnp.bfloat16)
            span = pl.ds(yy * dl_width, dl_width)
            near += jnp.dot(normed, w_own[span, :], preferred_element_type=jnp.float32)
            far += jnp.dot(normed, w_far[span, :], preferred_element_type=jnp.float32)
        shape = (4, CPC * 2, BLK_ROWS, dl_width)
        part[c, 0] = near.reshape(shape).astype(jnp.bfloat16)
        part[c, 1] = far.reshape(shape).astype(jnp.bfloat16)
        for j in range(1, 8):
            x_copy(c, j).start()

    def add(c):
        incoming = arrived.at[c, pl.ds(1, 7)]
        pltpu.make_async_copy(incoming, incoming, x_recv.at[c]).wait()
        for e in range(4):
            if e == 0:
                a = part[c, 0, xl * 2 + co]
            else:
                a = arrived[c, e]
            b = arrived[c, 4 + e]
            found[c, e] = (a.astype(jnp.float32) + b.astype(jnp.float32)).astype(jnp.bfloat16)

    def done(i):
        ahead = jnp.minimum(jnp.maximum((i - (FIRST - 1)) * BURST, 0), jnp.maximum(i - 1, 0))
        return jnp.minimum(ahead, chunks)

    def loop(i, carry):
        @pl.when(i == FIRST)
        def _():
            w_copy.wait_recv()
            w_share.start()
            load_w.wait()
            w_share.wait_recv()

        @pl.when(i >= FIRST)
        def _():
            lax.fori_loop(done(i - 1), done(i), lambda c, a: (multiply(c), a)[1], 0)

        @pl.when(i >= FIRST + 1)
        def _():
            lax.fori_loop(done(i - 2), done(i - 1), lambda c, a: (add(c), a)[1], 0)

        @pl.when(jnp.logical_and(i >= 1, i <= chunks))
        def _():
            relay(i - 1)

        @pl.when(i < chunks)
        def _():
            take(i)

        return carry

    lax.fori_loop(0, chunks + 3, loop, 0)

    def drain(c, carry):
        for side in range(2):
            y_copy(side, c).wait_send()
            relay_copy(side, c).wait_send()
        sent = stats.at[c, pl.ds(1, 7)]
        pltpu.make_async_copy(sent, sent, s_send.at[c]).wait()
        gone = arrived.at[c, pl.ds(1, 7)]
        pltpu.make_async_copy(gone, gone, x_send.at[c]).wait()
        return carry

    lax.fori_loop(0, chunks, drain, 0)

    def z_drain(q, carry):
        z_copy(q).wait_send()
        return carry

    lax.fori_loop(1, depth, z_drain, 0)
    w_copy.wait_send()
    w_share.wait_send()


def refresh(depth, order, rows, gain, weight):
    chunks = depth // CPC
    blocks, _, width = rows.shape
    bf16 = jnp.bfloat16
    dma = pltpu.SemaphoreType.DMA
    any_space = pl.BlockSpec(memory_space=pl.ANY)
    return pl.pallas_call(
        functools.partial(refresh_kernel, depth),
        out_shape=jax.ShapeDtypeStruct((chunks, 4, CPC * 2, BLK_ROWS, width), bf16),
        in_specs=[
            pl.BlockSpec(memory_space=pltpu.SMEM),
            any_space,
            pl.BlockSpec(memory_space=pltpu.VMEM),
            any_space,
        ],
        out_specs=pl.BlockSpec(memory_space=pltpu.VMEM),
        scratch_shapes=[
            pltpu.VMEM((blocks, BLK_ROWS, width), bf16),
            pltpu.VMEM((chunks, 4, CPC, 2, BLK_ROWS, width), bf16),
            pltpu.VMEM((4, chunks, 4, CPC, 2, BLK_ROWS, width), bf16),
            pltpu.VMEM((4 * width, width), bf16),
            pltpu.VMEM((4 * width, width), bf16),
            pltpu.VMEM((chunks, 8, 8, 128), jnp.float32),
            pltpu.VMEM((chunks, 2, 4, CPC * 2, BLK_ROWS, width), bf16),
            pltpu.VMEM((chunks, 8, CPC * 2, BLK_ROWS, width), bf16),
            dma,
            dma,
            dma((depth,)),
            dma((depth,)),
            dma((2, chunks)),
            dma((2, chunks)),
            dma((2, chunks)),
            dma((2, chunks)),
            dma((chunks,)),
            dma((chunks,)),
            dma((chunks,)),
            dma((chunks,)),
            dma,
            dma,
            dma,
            dma,
        ],
        compiler_params=pltpu.CompilerParams(
            collective_id=0, has_side_effects=True, vmem_limit_bytes=60 * 1024 * 1024
        ),
        name="refresh",
    )(order, rows, gain, weight)


def place_kernel(place, found, out):
    def step(p, carry):
        out[p] = found[place[p]]
        return carry

    lax.fori_loop(0, out.shape[0], step, 0, unroll=8)


def place_blocks(place, found):
    return pl.pallas_call(
        place_kernel,
        out_shape=jax.ShapeDtypeStruct(found.shape, found.dtype),
        in_specs=[pl.BlockSpec(memory_space=pltpu.SMEM), pl.BlockSpec(memory_space=pltpu.VMEM)],
        out_specs=pl.BlockSpec(memory_space=pltpu.VMEM),
        name="place",
    )(place, found)


def on_device(memory_rows, norm_gain, key_weight, owner_table):
    depth = lax.axis_size("grp") // 4
    row_count, width = memory_rows.shape
    order, place = tables(owner_table, depth)
    rows = memory_rows.reshape(row_count // BLK_ROWS, BLK_ROWS, width)
    found = refresh(depth, order, rows, norm_gain.reshape(1, -1), key_weight)
    out = place_blocks(place, found.reshape(row_count // BLK_ROWS, BLK_ROWS, width))
    return out.reshape(row_count, width)


def solution(mesh):
    in_specs = (P("grp", "tp"), P(), P(None, "tp"), P())
    out_specs = P("grp", "tp")
    return jax.shard_map(
        on_device, mesh=mesh, in_specs=in_specs, out_specs=out_specs, check_vma=False
    )
```

```python
import functools

import jax
import jax.numpy as jnp
from jax import lax
from jax.experimental import pallas as pl
from jax.experimental.pallas import tpu as pltpu
from jax.sharding import PartitionSpec as P

BLK_ROWS = 8
EPS = 1e-05
MESH = pl.DeviceIdType.MESH

VMEM_LIMIT = 60 * 1024 * 1024
FIRST = 8
BURST = 2
W_PARTS = 4


def class_shift(q, depth):
    return lax.rem(((q + 1) // 2) * (2 * lax.rem(q, 2) - 1) + depth, depth)


def flip(bit, by):
    return 1 - bit if by else bit


def order_table(own, z, depth):
    blocks = own.shape[1]
    down = jnp.broadcast_to(own, (blocks, blocks)).T
    lane = lax.broadcasted_iota(jnp.int32, (blocks, blocks), 1)
    block = lax.broadcasted_iota(jnp.int32, (blocks, blocks), 0)
    q = lane >> 3
    shift = ((q + 1) >> 1) * (2 * (q & 1) - 1)
    dest = ((z + shift + depth) & (depth - 1)) * 4 + ((lane >> 1) & 3)
    hit = down == dest
    low = jnp.min(jnp.where(hit, block, blocks - 1), axis=0, keepdims=True)
    high = jnp.max(jnp.where(hit, block, 0), axis=0, keepdims=True)
    return jnp.where((lane[0:1] & 1) == 0, low, high)


def place_table(table, g, depth):
    groups, blocks = table.shape
    z, xl, co = g // 4, lax.rem(g // 2, 2), lax.rem(g, 2)
    bits = blocks.bit_length() - 1
    lane = lax.broadcasted_iota(jnp.int32, (groups, blocks), 1)
    src = lax.broadcasted_iota(jnp.int32, (groups, blocks), 0)
    mine = (table >> bits) == g
    slot = table & (blocks - 1)
    column = jnp.where(mine, lane, blocks).astype(jnp.float32)
    first = jnp.min(column, axis=1, keepdims=True).astype(jnp.int32)
    slot_f = slot.astype(jnp.float32)
    slot_first = jnp.sum(jnp.where(lane == first, slot_f, 0.0), axis=1, keepdims=True)
    slot_both = jnp.sum(jnp.where(mine, slot_f, 0.0), axis=1, keepdims=True)
    slot_first, slot_last = slot_first.astype(jnp.int32), (slot_both - slot_first).astype(jnp.int32)
    back = (z - (src >> 2) + depth) & (depth - 1)
    q = jnp.where(back <= depth // 2, jnp.maximum(2 * back - 1, 0), 2 * (depth - back))
    dl = (((src >> 1) & 1) + xl) & 1
    dc = ((src & 1) + co) & 1
    at = (((q >> 1) * 4 + dl * 2 + dc) * 2 + (q & 1)) * 2
    spot = jnp.where(slot_first == lane, at, jnp.where(slot_last == lane, at + 1, 0))
    found = jnp.sum(spot.astype(jnp.float32), axis=0, keepdims=True).astype(jnp.int32)
    return jnp.minimum(found, blocks - 1)


def refresh_kernel(
    depth,
    x_hbm,
    gain_hbm,
    w_hbm,
    table_hbm,
    found,
    place,
    xin,
    gain,
    table,
    order_v,
    order,
    sorted_rows,
    gat,
    w_own,
    w_far,
    stats,
    normed,
    part,
    arrived,
    load_sem,
    send_sem,
    w_recv,
    z_recv,
    y_recv,
    r_recv,
    s_recv,
    x_recv,
):
    g, t = lax.axis_index("grp"), lax.axis_index("tp")
    z, xl, co = g // 4, lax.rem(g // 2, 2), lax.rem(g, 2)
    xh, y = t // 4, lax.rem(t, 4)
    chunks, pairs = depth, depth // 2
    dl_width = x_hbm.shape[-1]
    features = 8 * dl_width
    half_rows = 4 * dl_width
    rows_c = 64

    def device(zz, xxl, cc, xxh, yy):
        return {"grp": zz * 4 + xxl * 2 + cc, "tp": xxh * 4 + yy}

    w_start = pl.multiple_of(xh * half_rows, half_rows)
    load_table = pltpu.make_async_copy(table_hbm, table, load_sem.at[0])
    load_table.start()
    load = pltpu.make_async_copy(x_hbm, xin, load_sem.at[1])
    load.start()

    barrier = pltpu.get_barrier_semaphore()
    partners = 0
    for step in range(1, depth):
        pl.semaphore_signal(
            barrier, inc=1, device_id=device(lax.rem(z + step, depth), xl, co, xh, y), device_id_type=MESH
        )
        partners += 1
    for step in range(1, 8):
        pl.semaphore_signal(
            barrier, inc=1, device_id={"grp": g, "tp": lax.rem(t + step, 8)}, device_id_type=MESH
        )
        partners += 1
    for j in range(1, 8):
        if j == 4:
            continue
        pl.semaphore_signal(
            barrier,
            inc=1,
            device_id=device(z, flip(xl, (j // 2) % 2), flip(co, j % 2), flip(xh, j // 4), y),
            device_id_type=MESH,
        )
        partners += 1

    load_table.wait()
    own = table[pl.ds(g, 1), :] >> ((8 * depth).bit_length() - 1)
    order_v[...] = order_table(own, z, depth)
    load_order = pltpu.make_async_copy(order_v, order, load_sem.at[2])
    load_order.start()
    load_gain = pltpu.make_async_copy(gain_hbm, gain, load_sem.at[3])
    load_gain.start()
    load_w = pltpu.make_async_copy(w_hbm.at[pl.ds(w_start, half_rows)], w_own, load_sem.at[4])
    load_w.start()
    load_order.wait()
    load.wait()

    def sort_class(q):
        for e in range(8):
            sorted_rows[q, e] = xin[order[0, q * 8 + e]]

    def z_copy(q):
        return pltpu.make_async_remote_copy(
            src_ref=sorted_rows.at[q],
            dst_ref=gat.at[y, q],
            send_sem=send_sem.at[0],
            recv_sem=z_recv.at[q],
            device_id=device(lax.rem(z + class_shift(q, depth), depth), xl, co, xh, y),
            device_id_type=MESH,
        )

    ahead = min(2, depth - 1)
    for q in range(1, 1 + ahead):
        sort_class(q)
    pl.semaphore_wait(barrier, partners)

    w_rows = half_rows // 4
    w_run = w_rows // W_PARTS

    def w_span(l, c, k):
        return pl.ds(pl.multiple_of((l * 2 + c) * w_rows + k * w_run, w_run), w_run)

    def w_first(k):
        start = (1 - xh) * half_rows + ((1 - xl) * 2 + co) * w_rows + k * w_run
        return pltpu.make_async_remote_copy(
            src_ref=w_hbm.at[pl.ds(pl.multiple_of(start, w_run), w_run)],
            dst_ref=w_far.at[w_span(1 - xl, co, k)],
            send_sem=send_sem.at[1],
            recv_sem=w_recv.at[0, k],
            device_id=device(z, 1 - xl, co, 1 - xh, y),
            device_id_type=MESH,
        )

    def w_pass(kind, k):
        span = w_span(1 - xl if kind == 3 else xl, co, k)
        to = device(z, 1 - xl, co, xh, y) if kind == 1 else device(z, xl, 1 - co, xh, y)
        return pltpu.make_async_remote_copy(
            src_ref=w_far.at[span],
            dst_ref=w_far.at[span],
            send_sem=send_sem.at[1],
            recv_sem=w_recv.at[kind, k],
            device_id=to,
            device_id_type=MESH,
        )

    for k in range(W_PARTS):
        w_first(k).start()

    def z_start(q, carry):
        z_copy(q).start()

        @pl.when(q + ahead < depth)
        def _():
            sort_class(q + ahead)

        return carry

    lax.fori_loop(1, depth, z_start, 0)
    for e in range(8):
        gat[y, 0, e] = xin[order[0, e]]
    place[...] = place_table(table[...], g, depth)

    left, right = lax.rem(y + 3, 4), lax.rem(y + 1, 4)

    def y_copy(side, c):
        return pltpu.make_async_remote_copy(
            src_ref=gat.at[y, c],
            dst_ref=gat.at[y, c],
            send_sem=send_sem.at[2],
            recv_sem=y_recv.at[c],
            device_id=device(z, xl, co, xh, right if side == 0 else left),
            device_id_type=MESH,
        )

    def relay_copy(side, c):
        span = pl.ds(0, 4) if side == 0 else pl.ds(4, 4)
        piece = left if side == 0 else right
        return pltpu.make_async_remote_copy(
            src_ref=gat.at[piece, c, span],
            dst_ref=gat.at[piece, c, span],
            send_sem=send_sem.at[3],
            recv_sem=r_recv.at[c],
            device_id=device(z, xl, co, xh, right if side == 0 else left),
            device_id_type=MESH,
        )

    def stats_copy(c, step):
        return pltpu.make_async_remote_copy(
            src_ref=stats.at[c, 0],
            dst_ref=stats.at[c, step],
            send_sem=send_sem.at[4],
            recv_sem=s_recv.at[c],
            device_id={"grp": g, "tp": lax.rem(t + step, 8)},
            device_id_type=MESH,
        )

    def x_copy(p, j):
        dh, dl, dc = j // 4, (j // 2) % 2, j % 2
        to_l, to_c = flip(xl, dl), flip(co, dc)
        return pltpu.make_async_remote_copy(
            src_ref=part.at[p, dh, :, to_l * 2 + to_c],
            dst_ref=arrived.at[p, j],
            send_sem=send_sem.at[5],
            recv_sem=x_recv.at[p],
            device_id=device(z, to_l, to_c, flip(xh, dh), y),
            device_id_type=MESH,
        )

    def take(c):
        @pl.when(c > 0)
        def _():
            z_copy(c).wait_recv()

        y_copy(0, c).start()
        y_copy(1, c).start()
        v = gat[y, c].astype(jnp.float32).reshape(rows_c, dl_width)
        row_sum = jnp.sum(v, axis=1, keepdims=True)
        row_sq = jnp.sum(v * v, axis=1, keepdims=True)
        lane = lax.broadcasted_iota(jnp.int32, (rows_c, 128), 1)
        both = jnp.where(lane == 0, row_sum, jnp.where(lane == 1, row_sq, 0.0))
        stats[c, 0, :, pl.ds(0, rows_c)] = both.T[0:8, :]
        for step in range(1, 8):
            stats_copy(c, step).start()

    def all_of(ref, sem):
        pltpu.make_async_copy(ref, ref, sem).wait()

    def relay(c):
        all_of(gat.at[pl.ds(0, 2), c], y_recv.at[c])
        relay_copy(0, c).start()
        relay_copy(1, c).start()

    def multiply(p):
        means, scales = [], []
        for k in range(2):
            c = 2 * p + k
            all_of(gat.at[0, c], r_recv.at[c])
            all_of(stats.at[c, pl.ds(1, 7)], s_recv.at[c])
            total = jnp.sum(stats[c], axis=0)[:, 0:rows_c]
            mean = total[0:1] / features
            var = total[1:2] / features - mean * mean
            rstd = lax.rsqrt(var + EPS)
            sub = lax.broadcasted_iota(jnp.int32, (128, rows_c), 0)
            columns = jnp.where(sub == 0, mean, rstd).T
            mean_c, rstd_c = columns[:, 0:1], columns[:, 1:2]
            for yy in range(4):
                v = gat[yy, c].astype(jnp.float32).reshape(rows_c, dl_width)
                scale = gain[0:1, pl.ds(pl.multiple_of(w_start + yy * dl_width, dl_width), dl_width)]
                normed[pl.ds(k * rows_c, rows_c), pl.ds(yy * dl_width, dl_width)] = (
                    (v - mean_c) * rstd_c * scale
                ).astype(jnp.bfloat16)
        shape = (2, 4, 2, BLK_ROWS, dl_width)
        for dh, weight in ((1, w_far), (0, w_own)):
            keys = jnp.dot(normed[...], weight[...], preferred_element_type=jnp.float32)
            part[p, dh] = keys.reshape(shape).astype(jnp.bfloat16)
            for j in range(max(1, 4 * dh), 4 * dh + 4):
                x_copy(p, j).start()

    def add(p):
        all_of(arrived.at[p, pl.ds(1, 7)], x_recv.at[p])
        for e in range(4):
            a = part[p, 0, :, xl * 2 + co] if e == 0 else arrived[p, e]
            b = arrived[p, 4 + e]
            found[p, e] = (a.astype(jnp.float32) + b.astype(jnp.float32)).astype(jnp.bfloat16)

    def done(i):
        ready = jnp.minimum(jnp.maximum((i - (FIRST - 1)) * BURST, 0), jnp.maximum(i - 2, 0) // 2)
        return jnp.minimum(ready, pairs)

    def loop(i, carry):
        @pl.when(jnp.logical_and(i >= 2, i <= chunks + 1))
        def _():
            relay(i - 2)

        @pl.when(jnp.logical_and(i >= 2, i < 2 + W_PARTS))
        def _():
            w_first(i - 2).wait_recv()
            w_pass(1, i - 2).start()
            w_pass(2, i - 2).start()

        @pl.when(jnp.logical_and(i >= 4, i < 4 + W_PARTS))
        def _():
            w_pass(1, i - 4).wait_recv()
            w_pass(3, i - 4).start()

        @pl.when(i == FIRST)
        def _():
            load_w.wait()
            load_gain.wait()
            for k in range(W_PARTS):
                w_pass(2, k).wait_recv()
                w_pass(3, k).wait_recv()

        @pl.when(i >= FIRST)
        def _():
            lax.fori_loop(done(i - 1), done(i), lambda p, a: (multiply(p), a)[1], 0)

        @pl.when(i >= FIRST + 1)
        def _():
            lax.fori_loop(done(i - 2), done(i - 1), lambda p, a: (add(p), a)[1], 0)

        @pl.when(i < chunks)
        def _():
            take(i)

        return carry

    lax.fori_loop(0, chunks + 4, loop, 0)

    all_of(sorted_rows.at[pl.ds(1, depth - 1)], send_sem.at[0])
    all_of(w_own, send_sem.at[1])
    all_of(gat.at[pl.ds(0, 2)], send_sem.at[2])
    all_of(gat.at[0], send_sem.at[3])
    all_of(stats.at[:, pl.ds(1, 7)], send_sem.at[4])
    all_of(arrived.at[:, pl.ds(1, 7)], send_sem.at[5])


def refresh(depth, rows, gain, weight, table):
    chunks, pairs = depth, depth // 2
    blocks, _, width = rows.shape
    bf16 = jnp.bfloat16
    dma = pltpu.SemaphoreType.DMA
    hbm_space = pl.BlockSpec(memory_space=pltpu.HBM)
    return pl.pallas_call(
        functools.partial(refresh_kernel, depth),
        out_shape=[
            jax.ShapeDtypeStruct((pairs, 4, 2, 2, BLK_ROWS, width), bf16),
            jax.ShapeDtypeStruct((1, blocks), jnp.int32),
        ],
        in_specs=[hbm_space] * 4,
        out_specs=[pl.BlockSpec(memory_space=pltpu.VMEM)] * 2,
        scratch_shapes=[
            pltpu.VMEM((blocks, BLK_ROWS, width), bf16),
            pltpu.VMEM(gain.shape, jnp.float32),
            pltpu.VMEM(table.shape, jnp.int32),
            pltpu.VMEM((1, blocks), jnp.int32),
            pltpu.SMEM((1, blocks), jnp.int32),
            pltpu.VMEM((chunks, 8, BLK_ROWS, width), bf16),
            pltpu.VMEM((4, chunks, 8, BLK_ROWS, width), bf16),
            pltpu.VMEM((4 * width, width), bf16),
            pltpu.VMEM((4 * width, width), bf16),
            pltpu.VMEM((chunks, 8, 8, 128), jnp.float32),
            pltpu.VMEM((128, 4 * width), bf16),
            pltpu.VMEM((pairs, 2, 2, 4, 2, BLK_ROWS, width), bf16),
            pltpu.VMEM((pairs, 8, 2, 2, BLK_ROWS, width), bf16),
            dma((5,)),
            dma((6,)),
            dma((4, W_PARTS)),
            dma((depth,)),
            dma((chunks,)),
            dma((chunks,)),
            dma((chunks,)),
            dma((pairs,)),
        ],
        compiler_params=pltpu.CompilerParams(
            collective_id=0, has_side_effects=True, vmem_limit_bytes=VMEM_LIMIT
        ),
        name="refresh",
    )(rows, gain, weight, table)


def place_kernel(place, found, out, placed, out_sem):
    blocks = placed.shape[0]
    run = blocks // 4

    def step(p, carry):
        placed[p] = found[place[0, p]]
        return carry

    def save(part):
        span = pl.ds(part * run, run)
        return pltpu.make_async_copy(placed.at[span], out.at[span], out_sem.at[part])

    for part in range(4):
        lax.fori_loop(part * run, (part + 1) * run, step, 0, unroll=8)
        save(part).start()
    for part in range(4):
        save(part).wait()


def place_blocks(place, found):
    return pl.pallas_call(
        place_kernel,
        out_shape=jax.ShapeDtypeStruct(found.shape, found.dtype),
        in_specs=[pl.BlockSpec(memory_space=pltpu.SMEM), pl.BlockSpec(memory_space=pltpu.VMEM)],
        out_specs=pl.BlockSpec(memory_space=pl.ANY),
        scratch_shapes=[pltpu.VMEM(found.shape, found.dtype), pltpu.SemaphoreType.DMA((4,))],
        compiler_params=pltpu.CompilerParams(vmem_limit_bytes=VMEM_LIMIT),
        name="place",
    )(place, found)


def on_device(memory_rows, norm_gain, key_weight, owner_table):
    groups = lax.axis_size("grp")
    row_count, width = memory_rows.shape
    blocks = row_count // BLK_ROWS
    rows = memory_rows.reshape(blocks, BLK_ROWS, width)
    table = owner_table.reshape(groups, blocks)
    found, place = refresh(groups // 4, rows, norm_gain.reshape(1, -1), key_weight, table)
    out = place_blocks(place, found.reshape(blocks, BLK_ROWS, width))
    return out.reshape(row_count, width)


def solution(mesh):
    in_specs = (P("grp", "tp"), P(), P(None, "tp"), P())
    out_specs = P("grp", "tp")
    return jax.shard_map(
        on_device, mesh=mesh, in_specs=in_specs, out_specs=out_specs, check_vma=False
    )
```

```python
import functools

import jax
import jax.numpy as jnp
from jax import lax
from jax.experimental import pallas as pl
from jax.experimental.pallas import tpu as pltpu
from jax.sharding import PartitionSpec as P

BLK_ROWS = 8
EPS = 1e-05
MESH = pl.DeviceIdType.MESH

VMEM_LIMIT = 40 * 1024 * 1024
FIRST = 8
BURST = 2
LAG = 3
EARLY = 4
W_PARTS = 4


def shifts(depth):
    near = [n for step in range(1, depth // 2) for n in (step, -step)]
    far = [0, depth // 2] + near[::-1][: EARLY - 2]
    return far + near[: len(near) - (EARLY - 2)]


def look_up(index, values):
    out = jnp.zeros_like(index)
    for at, value in enumerate(values):
        out = jnp.where(index == at, value, out)
    return out


def flip(bit, by):
    return 1 - bit if by else bit


def order_table(own, z, depth):
    blocks = own.shape[1]
    down = jnp.broadcast_to(own, (blocks, blocks)).T
    lane = lax.broadcasted_iota(jnp.int32, (blocks, blocks), 1)
    block = lax.broadcasted_iota(jnp.int32, (blocks, blocks), 0)
    q = lane >> 3
    dest = ((z + look_up(q, shifts(depth)) + depth) & (depth - 1)) * 4 + ((lane >> 1) & 3)
    hit = down == dest
    low = jnp.min(jnp.where(hit, block, blocks - 1), axis=0, keepdims=True)
    high = jnp.max(jnp.where(hit, block, 0), axis=0, keepdims=True)
    return jnp.where((lane[0:1] & 1) == 0, low, high)


def place_table(table, g, depth):
    groups, blocks = table.shape
    z, xl, co = g // 4, lax.rem(g // 2, 2), lax.rem(g, 2)
    bits = blocks.bit_length() - 1
    lane = lax.broadcasted_iota(jnp.int32, (groups, blocks), 1)
    src = lax.broadcasted_iota(jnp.int32, (groups, blocks), 0)
    mine = (table >> bits) == g
    slot = table & (blocks - 1)
    column = jnp.where(mine, lane, blocks).astype(jnp.float32)
    first = jnp.min(column, axis=1, keepdims=True).astype(jnp.int32)
    slot_f = slot.astype(jnp.float32)
    slot_first = jnp.sum(jnp.where(lane == first, slot_f, 0.0), axis=1, keepdims=True)
    slot_both = jnp.sum(jnp.where(mine, slot_f, 0.0), axis=1, keepdims=True)
    slot_first, slot_last = slot_first.astype(jnp.int32), (slot_both - slot_first).astype(jnp.int32)
    back = (z - (src >> 2) + depth) & (depth - 1)
    chunk_of = {n % depth: q for q, n in enumerate(shifts(depth))}
    q = look_up(back, [chunk_of[n] for n in range(depth)])
    dl = (((src >> 1) & 1) + xl) & 1
    dc = ((src & 1) + co) & 1
    at = (((q >> 1) * 4 + dl * 2 + dc) * 2 + (q & 1)) * 2
    spot = jnp.where(slot_first == lane, at, jnp.where(slot_last == lane, at + 1, 0))
    found = jnp.sum(spot.astype(jnp.float32), axis=0, keepdims=True).astype(jnp.int32)
    return jnp.minimum(found, blocks - 1)


def refresh_kernel(
    depth,
    x_hbm,
    gain_hbm,
    w_hbm,
    table_hbm,
    found,
    place,
    xin,
    gain,
    table,
    order_v,
    order,
    sorted_rows,
    gat,
    w_own,
    w_far,
    stats,
    normed,
    part,
    arrived,
    leaving,
    landed,
    load_sem,
    send_sem,
    w_recv,
    z_recv,
    y_recv,
    r_recv,
    s_recv,
    x_recv,
):
    g, t = lax.axis_index("grp"), lax.axis_index("tp")
    z, xl, co = g // 4, lax.rem(g // 2, 2), lax.rem(g, 2)
    xh, y = t // 4, lax.rem(t, 4)
    chunks, pairs = depth, depth // 2
    dl_width = x_hbm.shape[-1]
    features = 8 * dl_width
    half_rows = 4 * dl_width
    rows_c = 64

    def device(zz, xxl, cc, xxh, yy):
        return {"grp": zz * 4 + xxl * 2 + cc, "tp": xxh * 4 + yy}

    w_start = pl.multiple_of(xh * half_rows, half_rows)
    load_table = pltpu.make_async_copy(table_hbm, table, load_sem.at[0])
    load_table.start()
    load = pltpu.make_async_copy(x_hbm, xin, load_sem.at[1])
    load.start()

    barrier = pltpu.get_barrier_semaphore()
    partners = 0
    for step in range(1, depth):
        pl.semaphore_signal(
            barrier, inc=1, device_id=device(lax.rem(z + step, depth), xl, co, xh, y), device_id_type=MESH
        )
        partners += 1
    for step in range(1, 8):
        pl.semaphore_signal(
            barrier, inc=1, device_id={"grp": g, "tp": lax.rem(t + step, 8)}, device_id_type=MESH
        )
        partners += 1
    for j in range(1, 8):
        if j == 4:
            continue
        pl.semaphore_signal(
            barrier,
            inc=1,
            device_id=device(z, flip(xl, (j // 2) % 2), flip(co, j % 2), flip(xh, j // 4), y),
            device_id_type=MESH,
        )
        partners += 1

    load_table.wait()
    own = table[pl.ds(g, 1), :] >> ((8 * depth).bit_length() - 1)
    order_v[...] = order_table(own, z, depth)
    load_order = pltpu.make_async_copy(order_v, order, load_sem.at[2])
    load_order.start()
    load_gain = pltpu.make_async_copy(gain_hbm, gain, load_sem.at[3])
    load_gain.start()
    load_w = pltpu.make_async_copy(w_hbm.at[pl.ds(w_start, half_rows)], w_own, load_sem.at[4])
    load_w.start()
    load_order.wait()
    load.wait()

    def sort_class(q):
        for e in range(8):
            sorted_rows[q, e] = xin[order[0, q * 8 + e]]

    def z_copy(q):
        return pltpu.make_async_remote_copy(
            src_ref=sorted_rows.at[q],
            dst_ref=gat.at[y, q],
            send_sem=send_sem.at[0],
            recv_sem=z_recv.at[q],
            device_id=device(lax.rem(z + shifts(depth)[q] + depth, depth), xl, co, xh, y),
            device_id_type=MESH,
        )

    for q in range(EARLY, EARLY + 2):
        sort_class(q)
    pl.semaphore_wait(barrier, partners)

    w_rows = half_rows // 4
    w_run = w_rows // W_PARTS

    def w_span(l, c, k):
        return pl.ds(pl.multiple_of((l * 2 + c) * w_rows + k * w_run, w_run), w_run)

    def w_first(k):
        start = (1 - xh) * half_rows + ((1 - xl) * 2 + co) * w_rows + k * w_run
        return pltpu.make_async_remote_copy(
            src_ref=w_hbm.at[pl.ds(pl.multiple_of(start, w_run), w_run)],
            dst_ref=w_far.at[w_span(1 - xl, co, k)],
            send_sem=send_sem.at[1],
            recv_sem=w_recv.at[0, k],
            device_id=device(z, 1 - xl, co, 1 - xh, y),
            device_id_type=MESH,
        )

    def w_pass(kind, k):
        span = w_span(1 - xl if kind == 3 else xl, co, k)
        to = device(z, 1 - xl, co, xh, y) if kind == 1 else device(z, xl, 1 - co, xh, y)
        return pltpu.make_async_remote_copy(
            src_ref=w_far.at[span],
            dst_ref=w_far.at[span],
            send_sem=send_sem.at[1],
            recv_sem=w_recv.at[kind, k],
            device_id=to,
            device_id_type=MESH,
        )

    for k in range(W_PARTS):
        w_first(k).start()

    for q in range(EARLY, depth):
        z_copy(q).start()
        if q + 2 < depth:
            sort_class(q + 2)
    for q in range(EARLY):
        for e in range(8):
            gat[y, q, e] = xin[order[0, q * 8 + e]]
    place[...] = place_table(table[...], g, depth)

    left, right = lax.rem(y + 3, 4), lax.rem(y + 1, 4)

    def y_copy(side, c):
        return pltpu.make_async_remote_copy(
            src_ref=gat.at[y, c],
            dst_ref=gat.at[y, c],
            send_sem=send_sem.at[2],
            recv_sem=y_recv.at[c],
            device_id=device(z, xl, co, xh, right if side == 0 else left),
            device_id_type=MESH,
        )

    def relay_copy(side, c):
        span = pl.ds(0, 4) if side == 0 else pl.ds(4, 4)
        piece = left if side == 0 else right
        return pltpu.make_async_remote_copy(
            src_ref=gat.at[piece, c, span],
            dst_ref=gat.at[piece, c, span],
            send_sem=send_sem.at[3],
            recv_sem=r_recv.at[c],
            device_id=device(z, xl, co, xh, right if side == 0 else left),
            device_id_type=MESH,
        )

    def stats_copy(c, step):
        return pltpu.make_async_remote_copy(
            src_ref=stats.at[c, 0],
            dst_ref=stats.at[c, step],
            send_sem=send_sem.at[4],
            recv_sem=s_recv.at[c],
            device_id={"grp": g, "tp": lax.rem(t + step, 8)},
            device_id_type=MESH,
        )

    def x_copy(p, j):
        dh, dl, dc = j // 4, (j // 2) % 2, j % 2
        to_l, to_c = flip(xl, dl), flip(co, dc)
        return pltpu.make_async_remote_copy(
            src_ref=part.at[p, dh, :, to_l * 2 + to_c],
            dst_ref=arrived.at[p, j],
            send_sem=send_sem.at[5],
            recv_sem=x_recv.at[p],
            device_id=device(z, to_l, to_c, flip(xh, dh), y),
            device_id_type=MESH,
        )

    def all_of(ref, sem):
        pltpu.make_async_copy(ref, ref, sem).wait()

    def key_copy(q):
        return pltpu.make_async_remote_copy(
            src_ref=leaving.at[q // 2, :, q % 2],
            dst_ref=landed.at[q // 2, :, q % 2],
            send_sem=send_sem.at[0],
            recv_sem=z_recv.at[q],
            device_id=device(lax.rem(z + shifts(depth)[q] + depth, depth), xl, co, xh, y),
            device_id_type=MESH,
        )

    def take(c):
        @pl.when(c >= EARLY)
        def _():
            all_of(gat.at[0, c], z_recv.at[c])

        y_copy(0, c).start()
        y_copy(1, c).start()
        v = gat[y, c].astype(jnp.float32).reshape(rows_c, dl_width)
        row_sum = jnp.sum(v, axis=1, keepdims=True)
        row_sq = jnp.sum(v * v, axis=1, keepdims=True)
        lane = lax.broadcasted_iota(jnp.int32, (rows_c, 128), 1)
        both = jnp.where(lane == 0, row_sum, jnp.where(lane == 1, row_sq, 0.0))
        flat = both.T
        stats[c, 0, :, pl.ds(0, rows_c)] = flat[0:1, :]
        stats[c, 0, :, pl.ds(rows_c, rows_c)] = flat[1:2, :]
        for step in range(1, 8):
            stats_copy(c, step).start()

    def relay(c):
        all_of(gat.at[pl.ds(0, 2), c], y_recv.at[c])
        relay_copy(0, c).start()
        relay_copy(1, c).start()

    def multiply(p):
        means, scales = [], []
        for k in range(2):
            c = 2 * p + k
            all_of(gat.at[0, c], r_recv.at[c])
            all_of(stats.at[c, pl.ds(1, 7)], s_recv.at[c])
            total = jnp.sum(stats[c], axis=0)
            mean = total[:, 0:rows_c] / features
            var = total[:, rows_c : 2 * rows_c] / features - mean * mean
            rstd = lax.rsqrt(var + EPS)
            sub = lax.broadcasted_iota(jnp.int32, (128, rows_c), 0)
            columns = jnp.where(sub == 0, mean, rstd).T
            mean_c, rstd_c = columns[:, 0:1], columns[:, 1:2]
            for yy in range(4):
                v = gat[yy, c].astype(jnp.float32).reshape(rows_c, dl_width)
                scale = gain[0:1, pl.ds(pl.multiple_of(w_start + yy * dl_width, dl_width), dl_width)]
                normed[pl.ds(k * rows_c, rows_c), pl.ds(yy * dl_width, dl_width)] = (
                    (v - mean_c) * rstd_c * scale
                ).astype(jnp.bfloat16)
        shape = (2, 4, 2, BLK_ROWS, dl_width)
        for dh, weight in ((1, w_far), (0, w_own)):
            keys = jnp.dot(normed[...], weight[...], preferred_element_type=jnp.float32)
            part[p, dh] = keys.reshape(shape).astype(jnp.bfloat16)
            for j in range(max(1, 4 * dh), 4 * dh + 4):
                x_copy(p, j).start()

    def add(p):
        all_of(arrived.at[p, pl.ds(1, 7)], x_recv.at[p])
        for e in range(4):
            a = part[p, 0, :, xl * 2 + co] if e == 0 else arrived[p, e]
            b = arrived[p, 4 + e]
            keys = (a.astype(jnp.float32) + b.astype(jnp.float32)).astype(jnp.bfloat16)
            found[p, e] = keys

            @pl.when(p < EARLY // 2)
            def _():
                leaving[p, e] = keys

        for early in range(EARLY // 2):

            @pl.when(p == early)
            def _():
                for q in range(max(1, 2 * early), 2 * early + 2):
                    key_copy(q).start()

    def done(i):
        ready = jnp.minimum(jnp.maximum((i - (FIRST - 1)) * BURST, 0), jnp.maximum(i - 2, 0) // 2)
        return jnp.minimum(ready, pairs)

    def loop(i, carry):
        @pl.when(jnp.logical_and(i >= 2, i < 2 + W_PARTS))
        def _():
            w_first(i - 2).wait_recv()
            w_pass(1, i - 2).start()
            w_pass(2, i - 2).start()

        @pl.when(jnp.logical_and(i >= 4, i < 4 + W_PARTS))
        def _():
            w_pass(1, i - 4).wait_recv()
            w_pass(3, i - 4).start()

        @pl.when(i == FIRST)
        def _():
            load_w.wait()
            load_gain.wait()
            for k in range(W_PARTS):
                w_pass(2, k).wait_recv()
                w_pass(3, k).wait_recv()

        @pl.when(i >= FIRST)
        def _():
            lax.fori_loop(done(i - 1), done(i), lambda p, a: (multiply(p), a)[1], 0)

        @pl.when(jnp.logical_and(i >= 2, i <= chunks + 1))
        def _():
            relay(i - 2)

        @pl.when(i >= FIRST + LAG)
        def _():
            lax.fori_loop(done(i - LAG - 1), done(i - LAG), lambda p, a: (add(p), a)[1], 0)

        @pl.when(i < chunks)
        def _():
            take(i)

        return carry

    lax.fori_loop(0, chunks + 3 + LAG, loop, 0)

    for q in range(1, EARLY):
        all_of(gat.at[0, q], z_recv.at[q])
        found[q // 2, :, q % 2] = landed[q // 2, :, q % 2]

    all_of(sorted_rows.at[pl.ds(1, depth - 1)], send_sem.at[0])
    all_of(w_own, send_sem.at[1])
    all_of(gat.at[pl.ds(0, 2)], send_sem.at[2])
    all_of(gat.at[0], send_sem.at[3])
    all_of(stats.at[:, pl.ds(1, 7)], send_sem.at[4])
    all_of(arrived.at[:, pl.ds(1, 7)], send_sem.at[5])


def refresh(depth, rows, gain, weight, table):
    chunks, pairs = depth, depth // 2
    blocks, _, width = rows.shape
    bf16 = jnp.bfloat16
    dma = pltpu.SemaphoreType.DMA
    hbm_space = pl.BlockSpec(memory_space=pltpu.HBM)
    return pl.pallas_call(
        functools.partial(refresh_kernel, depth),
        out_shape=[
            jax.ShapeDtypeStruct((pairs, 4, 2, 2, BLK_ROWS, width), bf16),
            jax.ShapeDtypeStruct((1, blocks), jnp.int32),
        ],
        in_specs=[hbm_space] * 4,
        out_specs=[pl.BlockSpec(memory_space=pltpu.VMEM)] * 2,
        scratch_shapes=[
            pltpu.VMEM((blocks, BLK_ROWS, width), bf16),
            pltpu.VMEM(gain.shape, jnp.float32),
            pltpu.VMEM(table.shape, jnp.int32),
            pltpu.VMEM((1, blocks), jnp.int32),
            pltpu.SMEM((1, blocks), jnp.int32),
            pltpu.VMEM((chunks, 8, BLK_ROWS, width), bf16),
            pltpu.VMEM((4, chunks, 8, BLK_ROWS, width), bf16),
            pltpu.VMEM((4 * width, width), bf16),
            pltpu.VMEM((4 * width, width), bf16),
            pltpu.VMEM((chunks, 8, 1, 128), jnp.float32),
            pltpu.VMEM((128, 4 * width), bf16),
            pltpu.VMEM((pairs, 2, 2, 4, 2, BLK_ROWS, width), bf16),
            pltpu.VMEM((pairs, 8, 2, 2, BLK_ROWS, width), bf16),
            pltpu.VMEM((EARLY // 2, 4, 2, 2, BLK_ROWS, width), bf16),
            pltpu.VMEM((EARLY // 2, 4, 2, 2, BLK_ROWS, width), bf16),
            dma((5,)),
            dma((6,)),
            dma((4, W_PARTS)),
            dma((depth,)),
            dma((chunks,)),
            dma((chunks,)),
            dma((chunks,)),
            dma((pairs,)),
        ],
        compiler_params=pltpu.CompilerParams(
            collective_id=0, has_side_effects=True, vmem_limit_bytes=VMEM_LIMIT
        ),
        name="refresh",
    )(*(pltpu.with_memory_space_constraint(a, pltpu.HBM) for a in (rows, gain, weight, table)))


def place_kernel(place, found, out, placed, out_sem):
    blocks = placed.shape[0]
    run = blocks // 4

    def step(p, carry):
        placed[p] = found[place[0, p]]
        return carry

    def save(part):
        span = pl.ds(part * run, run)
        return pltpu.make_async_copy(placed.at[span], out.at[span], out_sem.at[part])

    for part in range(4):
        lax.fori_loop(part * run, (part + 1) * run, step, 0, unroll=8)
        save(part).start()
    for part in range(4):
        save(part).wait()


def place_blocks(place, found):
    return pl.pallas_call(
        place_kernel,
        out_shape=jax.ShapeDtypeStruct(found.shape, found.dtype),
        in_specs=[pl.BlockSpec(memory_space=pltpu.SMEM), pl.BlockSpec(memory_space=pltpu.VMEM)],
        out_specs=pl.BlockSpec(memory_space=pl.ANY),
        scratch_shapes=[pltpu.VMEM(found.shape, found.dtype), pltpu.SemaphoreType.DMA((4,))],
        compiler_params=pltpu.CompilerParams(vmem_limit_bytes=4 * 1024 * 1024),
        name="place",
    )(place, found)


def on_device(memory_rows, norm_gain, key_weight, owner_table):
    groups = lax.axis_size("grp")
    row_count, width = memory_rows.shape
    blocks = row_count // BLK_ROWS
    rows = memory_rows.reshape(blocks, BLK_ROWS, width)
    table = owner_table.reshape(groups, blocks)
    found, place = refresh(groups // 4, rows, norm_gain.reshape(1, -1), key_weight, table)
    out = place_blocks(place, found.reshape(blocks, BLK_ROWS, width))
    return out.reshape(row_count, width)


def solution(mesh):
    in_specs = (P("grp", "tp"), P(), P(None, "tp"), P())
    out_specs = P("grp", "tp")
    return jax.shard_map(
        on_device, mesh=mesh, in_specs=in_specs, out_specs=out_specs, check_vma=False
    )
```

```python
import functools

import jax
import jax.numpy as jnp
from jax import lax
from jax.experimental import pallas as pl
from jax.experimental.pallas import tpu as pltpu
from jax.sharding import PartitionSpec as P

BLK_ROWS = 8
EPS = 1e-05
MESH = pl.DeviceIdType.MESH

VMEM_LIMIT = 40 * 1024 * 1024
FIRST = 8
BURST = 3
LAG = 3
EARLY = 4
LEAD = 3
RELAY = 0
MATMUL = 3
W_ONE = 2
W_TWO = 4
W_PARTS = 4


def shifts(depth):
    near = [n for step in range(1, depth // 2) for n in (step, -step)]
    far = [0, depth // 2] + near[::-1][: EARLY - 2]
    return far + near[: len(near) - (EARLY - 2)]


def look_up(index, values):
    out = jnp.zeros_like(index)
    for at, value in enumerate(values):
        out = jnp.where(index == at, value, out)
    return out


def flip(bit, by):
    return 1 - bit if by else bit


def order_table(own, z, depth):
    blocks = own.shape[1]
    down = jnp.broadcast_to(own, (blocks, blocks)).T
    lane = lax.broadcasted_iota(jnp.int32, (blocks, blocks), 1)
    block = lax.broadcasted_iota(jnp.int32, (blocks, blocks), 0)
    q = lane >> 3
    dest = ((z + look_up(q, shifts(depth)) + depth) & (depth - 1)) * 4 + ((lane >> 1) & 3)
    hit = down == dest
    low = jnp.min(jnp.where(hit, block, blocks - 1), axis=0, keepdims=True)
    high = jnp.max(jnp.where(hit, block, 0), axis=0, keepdims=True)
    return jnp.where((lane[0:1] & 1) == 0, low, high)


def place_table(table, g, depth):
    groups, blocks = table.shape
    z, xl, co = g // 4, lax.rem(g // 2, 2), lax.rem(g, 2)
    bits = blocks.bit_length() - 1
    lane = lax.broadcasted_iota(jnp.int32, (groups, blocks), 1)
    src = lax.broadcasted_iota(jnp.int32, (groups, blocks), 0)
    mine = (table >> bits) == g
    slot = table & (blocks - 1)
    column = jnp.where(mine, lane, blocks).astype(jnp.float32)
    first = jnp.min(column, axis=1, keepdims=True).astype(jnp.int32)
    slot_f = slot.astype(jnp.float32)
    slot_first = jnp.sum(jnp.where(lane == first, slot_f, 0.0), axis=1, keepdims=True)
    slot_both = jnp.sum(jnp.where(mine, slot_f, 0.0), axis=1, keepdims=True)
    slot_first, slot_last = slot_first.astype(jnp.int32), (slot_both - slot_first).astype(jnp.int32)
    back = (z - (src >> 2) + depth) & (depth - 1)
    chunk_of = {n % depth: q for q, n in enumerate(shifts(depth))}
    q = look_up(back, [chunk_of[n] for n in range(depth)])
    dl = (((src >> 1) & 1) + xl) & 1
    dc = ((src & 1) + co) & 1
    at = (((q >> 1) * 4 + dl * 2 + dc) * 2 + (q & 1)) * 2
    spot = jnp.where(slot_first == lane, at, jnp.where(slot_last == lane, at + 1, 0))
    found = jnp.sum(spot.astype(jnp.float32), axis=0, keepdims=True).astype(jnp.int32)
    return jnp.minimum(found, blocks - 1)


def refresh_kernel(
    depth,
    x_hbm,
    gain_hbm,
    w_hbm,
    table_hbm,
    found,
    place,
    xin,
    gain,
    table,
    order_v,
    order,
    sorted_rows,
    gat,
    w_own,
    w_far,
    stats,
    normed,
    part,
    arrived,
    leaving,
    landed,
    load_sem,
    send_sem,
    w_recv,
    z_recv,
    y_recv,
    r_recv,
    s_recv,
    x_recv,
):
    g, t = lax.axis_index("grp"), lax.axis_index("tp")
    z, xl, co = g // 4, lax.rem(g // 2, 2), lax.rem(g, 2)
    xh, y = t // 4, lax.rem(t, 4)
    chunks, pairs = depth, depth // 2
    dl_width = x_hbm.shape[-1]
    features = 8 * dl_width
    half_rows = 4 * dl_width
    rows_c = 64

    def device(zz, xxl, cc, xxh, yy):
        return {"grp": zz * 4 + xxl * 2 + cc, "tp": xxh * 4 + yy}

    w_start = pl.multiple_of(xh * half_rows, half_rows)
    load_table = pltpu.make_async_copy(table_hbm, table, load_sem.at[0])
    load_table.start()
    load = pltpu.make_async_copy(x_hbm, xin, load_sem.at[1])
    load.start()

    barrier = pltpu.get_barrier_semaphore()
    partners = 0
    for step in range(1, depth):
        pl.semaphore_signal(
            barrier, inc=1, device_id=device(lax.rem(z + step, depth), xl, co, xh, y), device_id_type=MESH
        )
        partners += 1
    for step in range(1, 8):
        pl.semaphore_signal(
            barrier, inc=1, device_id={"grp": g, "tp": lax.rem(t + step, 8)}, device_id_type=MESH
        )
        partners += 1
    for j in range(1, 8):
        if j == 4:
            continue
        pl.semaphore_signal(
            barrier,
            inc=1,
            device_id=device(z, flip(xl, (j // 2) % 2), flip(co, j % 2), flip(xh, j // 4), y),
            device_id_type=MESH,
        )
        partners += 1

    load_table.wait()
    own = table[pl.ds(g, 1), :] >> ((8 * depth).bit_length() - 1)
    order_v[...] = order_table(own, z, depth)
    load_order = pltpu.make_async_copy(order_v, order, load_sem.at[2])
    load_order.start()
    load_gain = pltpu.make_async_copy(gain_hbm, gain, load_sem.at[3])
    load_gain.start()
    load_w = pltpu.make_async_copy(w_hbm.at[pl.ds(w_start, half_rows)], w_own, load_sem.at[4])
    load_w.start()
    load_order.wait()
    load.wait()

    def sort_class(q):
        for e in range(8):
            sorted_rows[q, e] = xin[order[0, q * 8 + e]]

    def z_copy(q):
        return pltpu.make_async_remote_copy(
            src_ref=sorted_rows.at[q],
            dst_ref=gat.at[y, q],
            send_sem=send_sem.at[0],
            recv_sem=z_recv.at[q],
            device_id=device(lax.rem(z + shifts(depth)[q] + depth, depth), xl, co, xh, y),
            device_id_type=MESH,
        )

    for q in range(EARLY, EARLY + 2):
        sort_class(q)
    pl.semaphore_wait(barrier, partners)

    w_rows = half_rows // 4
    w_run = w_rows // W_PARTS

    def w_span(l, c, k):
        return pl.ds(pl.multiple_of((l * 2 + c) * w_rows + k * w_run, w_run), w_run)

    def w_first(k):
        start = (1 - xh) * half_rows + ((1 - xl) * 2 + co) * w_rows + k * w_run
        return pltpu.make_async_remote_copy(
            src_ref=w_hbm.at[pl.ds(pl.multiple_of(start, w_run), w_run)],
            dst_ref=w_far.at[w_span(1 - xl, co, k)],
            send_sem=send_sem.at[1],
            recv_sem=w_recv.at[0, k],
            device_id=device(z, 1 - xl, co, 1 - xh, y),
            device_id_type=MESH,
        )

    def w_pass(kind, k):
        span = w_span(1 - xl if kind == 3 else xl, co, k)
        to = device(z, 1 - xl, co, xh, y) if kind == 1 else device(z, xl, 1 - co, xh, y)
        return pltpu.make_async_remote_copy(
            src_ref=w_far.at[span],
            dst_ref=w_far.at[span],
            send_sem=send_sem.at[1],
            recv_sem=w_recv.at[kind, k],
            device_id=to,
            device_id_type=MESH,
        )

    for k in range(W_PARTS):
        w_first(k).start()

    for q in range(EARLY, depth):
        z_copy(q).start()
        if q + 2 < depth:
            sort_class(q + 2)
    for q in range(EARLY):
        for e in range(8):
            gat[y, q, e] = xin[order[0, q * 8 + e]]
    place[...] = place_table(table[...], g, depth)

    left, right = lax.rem(y + 3, 4), lax.rem(y + 1, 4)

    def y_copy(side, c):
        return pltpu.make_async_remote_copy(
            src_ref=gat.at[y, c],
            dst_ref=gat.at[y, c],
            send_sem=send_sem.at[2],
            recv_sem=y_recv.at[c],
            device_id=device(z, xl, co, xh, right if side == 0 else left),
            device_id_type=MESH,
        )

    def relay_copy(side, c):
        span = pl.ds(0, 4) if side == 0 else pl.ds(4, 4)
        piece = left if side == 0 else right
        return pltpu.make_async_remote_copy(
            src_ref=gat.at[piece, c, span],
            dst_ref=gat.at[piece, c, span],
            send_sem=send_sem.at[3],
            recv_sem=r_recv.at[c],
            device_id=device(z, xl, co, xh, right if side == 0 else left),
            device_id_type=MESH,
        )

    def stats_copy(c, step):
        return pltpu.make_async_remote_copy(
            src_ref=stats.at[c, 0],
            dst_ref=stats.at[c, step],
            send_sem=send_sem.at[4],
            recv_sem=s_recv.at[c],
            device_id={"grp": g, "tp": lax.rem(t + step, 8)},
            device_id_type=MESH,
        )

    def x_copy(p, j):
        dh, dl, dc = j // 4, (j // 2) % 2, j % 2
        to_l, to_c = flip(xl, dl), flip(co, dc)
        return pltpu.make_async_remote_copy(
            src_ref=part.at[p, dh, :, to_l * 2 + to_c],
            dst_ref=arrived.at[p, j],
            send_sem=send_sem.at[5],
            recv_sem=x_recv.at[p],
            device_id=device(z, to_l, to_c, flip(xh, dh), y),
            device_id_type=MESH,
        )

    def all_of(ref, sem):
        pltpu.make_async_copy(ref, ref, sem).wait()

    def key_copy(q):
        return pltpu.make_async_remote_copy(
            src_ref=leaving.at[q // 2, :, q % 2],
            dst_ref=landed.at[q // 2, :, q % 2],
            send_sem=send_sem.at[0],
            recv_sem=z_recv.at[q],
            device_id=device(lax.rem(z + shifts(depth)[q] + depth, depth), xl, co, xh, y),
            device_id_type=MESH,
        )

    def take(c):
        @pl.when(c >= EARLY)
        def _():
            all_of(gat.at[0, c], z_recv.at[c])

        y_copy(0, c).start()
        y_copy(1, c).start()
        v = gat[y, c].astype(jnp.float32).reshape(rows_c, dl_width)
        row_sum = jnp.sum(v, axis=1, keepdims=True)
        row_sq = jnp.sum(v * v, axis=1, keepdims=True)
        lane = lax.broadcasted_iota(jnp.int32, (rows_c, 128), 1)
        both = jnp.where(lane == 0, row_sum, jnp.where(lane == 1, row_sq, 0.0))
        flat = both.T
        stats[c, 0, :, pl.ds(0, rows_c)] = flat[0:1, :]
        stats[c, 0, :, pl.ds(rows_c, rows_c)] = flat[1:2, :]
        for step in range(1, 8):
            stats_copy(c, step).start()

    def relay(c):
        all_of(gat.at[pl.ds(0, 2), c], y_recv.at[c])
        relay_copy(0, c).start()
        relay_copy(1, c).start()

    def multiply(p):
        means, scales = [], []
        for k in range(2):
            c = 2 * p + k
            all_of(gat.at[0, c], r_recv.at[c])
            all_of(stats.at[c, pl.ds(1, 7)], s_recv.at[c])
            total = jnp.sum(stats[c], axis=0)
            mean = total[:, 0:rows_c] / features
            var = total[:, rows_c : 2 * rows_c] / features - mean * mean
            rstd = lax.rsqrt(var + EPS)
            sub = lax.broadcasted_iota(jnp.int32, (128, rows_c), 0)
            columns = jnp.where(sub == 0, mean, rstd).T
            mean_c, rstd_c = columns[:, 0:1], columns[:, 1:2]
            for yy in range(4):
                v = gat[yy, c].astype(jnp.float32).reshape(rows_c, dl_width)
                scale = gain[0:1, pl.ds(pl.multiple_of(w_start + yy * dl_width, dl_width), dl_width)]
                normed[pl.ds(k * rows_c, rows_c), pl.ds(yy * dl_width, dl_width)] = (
                    (v - mean_c) * rstd_c * scale
                ).astype(jnp.bfloat16)
        shape = (2, 4, 2, BLK_ROWS, dl_width)
        for dh, weight in ((1, w_far), (0, w_own)):
            keys = jnp.dot(normed[...], weight[...], preferred_element_type=jnp.float32)
            part[p, dh] = keys.reshape(shape).astype(jnp.bfloat16)
            for j in range(max(1, 4 * dh), 4 * dh + 4):
                x_copy(p, j).start()

    def add(p):
        all_of(arrived.at[p, pl.ds(1, 7)], x_recv.at[p])
        for e in range(4):
            a = part[p, 0, :, xl * 2 + co] if e == 0 else arrived[p, e]
            b = arrived[p, 4 + e]
            keys = (a.astype(jnp.float32) + b.astype(jnp.float32)).astype(jnp.bfloat16)
            found[p, e] = keys

            @pl.when(p < EARLY // 2)
            def _():
                leaving[p, e] = keys

        for early in range(EARLY // 2):

            @pl.when(p == early)
            def _():
                for q in range(max(1, 2 * early), 2 * early + 2):
                    key_copy(q).start()

    def done(i):
        ready = jnp.minimum(jnp.maximum((i - (FIRST - 1)) * BURST, 0), jnp.maximum(i - (MATMUL - 1), 0) // 2)
        return jnp.minimum(ready, pairs)

    def loop(i, carry):
        @pl.when(jnp.logical_and(i >= W_ONE, i < W_ONE + W_PARTS))
        def _():
            w_first(i - W_ONE).wait_recv()
            w_pass(1, i - W_ONE).start()
            w_pass(2, i - W_ONE).start()

        @pl.when(jnp.logical_and(i >= W_TWO, i < W_TWO + W_PARTS))
        def _():
            w_pass(1, i - W_TWO).wait_recv()
            w_pass(3, i - W_TWO).start()

        @pl.when(i == FIRST)
        def _():
            load_w.wait()
            load_gain.wait()
            for k in range(W_PARTS):
                w_pass(2, k).wait_recv()
                w_pass(3, k).wait_recv()

        @pl.when(i >= FIRST)
        def _():
            lax.fori_loop(done(i - 1), done(i), lambda p, a: (multiply(p), a)[1], 0)

        @pl.when(jnp.logical_and(i >= RELAY, i < chunks + RELAY))
        def _():
            relay(i - RELAY)

        @pl.when(i >= FIRST + LAG)
        def _():
            lax.fori_loop(done(i - LAG - 1), done(i - LAG), lambda p, a: (add(p), a)[1], 0)

        @pl.when(i < chunks - LEAD)
        def _():
            take(i + LEAD)

        return carry

    lax.fori_loop(0, LEAD, lambda c, a: (take(c), a)[1], 0)
    lax.fori_loop(0, chunks + MATMUL + LAG, loop, 0)

    for q in range(1, EARLY):
        all_of(gat.at[0, q], z_recv.at[q])
        found[q // 2, :, q % 2] = landed[q // 2, :, q % 2]

    all_of(sorted_rows.at[pl.ds(1, depth - 1)], send_sem.at[0])
    all_of(w_own, send_sem.at[1])
    all_of(gat.at[pl.ds(0, 2)], send_sem.at[2])
    all_of(gat.at[0], send_sem.at[3])
    all_of(stats.at[:, pl.ds(1, 7)], send_sem.at[4])
    all_of(arrived.at[:, pl.ds(1, 7)], send_sem.at[5])


def refresh(depth, rows, gain, weight, table):
    chunks, pairs = depth, depth // 2
    blocks, _, width = rows.shape
    bf16 = jnp.bfloat16
    dma = pltpu.SemaphoreType.DMA
    hbm_space = pl.BlockSpec(memory_space=pltpu.HBM)
    return pl.pallas_call(
        functools.partial(refresh_kernel, depth),
        out_shape=[
            jax.ShapeDtypeStruct((pairs, 4, 2, 2, BLK_ROWS, width), bf16),
            jax.ShapeDtypeStruct((1, blocks), jnp.int32),
        ],
        in_specs=[hbm_space] * 4,
        out_specs=[pl.BlockSpec(memory_space=pltpu.VMEM)] * 2,
        scratch_shapes=[
            pltpu.VMEM((blocks, BLK_ROWS, width), bf16),
            pltpu.VMEM(gain.shape, jnp.float32),
            pltpu.VMEM(table.shape, jnp.int32),
            pltpu.VMEM((1, blocks), jnp.int32),
            pltpu.SMEM((1, blocks), jnp.int32),
            pltpu.VMEM((chunks, 8, BLK_ROWS, width), bf16),
            pltpu.VMEM((4, chunks, 8, BLK_ROWS, width), bf16),
            pltpu.VMEM((4 * width, width), bf16),
            pltpu.VMEM((4 * width, width), bf16),
            pltpu.VMEM((chunks, 8, 1, 128), jnp.float32),
            pltpu.VMEM((128, 4 * width), bf16),
            pltpu.VMEM((pairs, 2, 2, 4, 2, BLK_ROWS, width), bf16),
            pltpu.VMEM((pairs, 8, 2, 2, BLK_ROWS, width), bf16),
            pltpu.VMEM((EARLY // 2, 4, 2, 2, BLK_ROWS, width), bf16),
            pltpu.VMEM((EARLY // 2, 4, 2, 2, BLK_ROWS, width), bf16),
            dma((5,)),
            dma((6,)),
            dma((4, W_PARTS)),
            dma((depth,)),
            dma((chunks,)),
            dma((chunks,)),
            dma((chunks,)),
            dma((pairs,)),
        ],
        compiler_params=pltpu.CompilerParams(
            collective_id=0, has_side_effects=True, vmem_limit_bytes=VMEM_LIMIT
        ),
        name="refresh",
    )(*(pltpu.with_memory_space_constraint(a, pltpu.HBM) for a in (rows, gain, weight, table)))


def place_kernel(place, found, out, placed, out_sem):
    blocks = placed.shape[0]
    run = blocks // 4

    def step(p, carry):
        placed[p] = found[place[0, p]]
        return carry

    def save(part):
        span = pl.ds(part * run, run)
        return pltpu.make_async_copy(placed.at[span], out.at[span], out_sem.at[part])

    for part in range(4):
        lax.fori_loop(part * run, (part + 1) * run, step, 0, unroll=8)
        save(part).start()
    for part in range(4):
        save(part).wait()


def place_blocks(place, found):
    return pl.pallas_call(
        place_kernel,
        out_shape=jax.ShapeDtypeStruct(found.shape, found.dtype),
        in_specs=[pl.BlockSpec(memory_space=pltpu.SMEM), pl.BlockSpec(memory_space=pltpu.VMEM)],
        out_specs=pl.BlockSpec(memory_space=pl.ANY),
        scratch_shapes=[pltpu.VMEM(found.shape, found.dtype), pltpu.SemaphoreType.DMA((4,))],
        compiler_params=pltpu.CompilerParams(vmem_limit_bytes=4 * 1024 * 1024),
        name="place",
    )(place, found)


def on_device(memory_rows, norm_gain, key_weight, owner_table):
    groups = lax.axis_size("grp")
    row_count, width = memory_rows.shape
    blocks = row_count // BLK_ROWS
    rows = memory_rows.reshape(blocks, BLK_ROWS, width)
    table = owner_table.reshape(groups, blocks)
    found, place = refresh(groups // 4, rows, norm_gain.reshape(1, -1), key_weight, table)
    out = place_blocks(place, found.reshape(blocks, BLK_ROWS, width))
    return out.reshape(row_count, width)


def solution(mesh):
    in_specs = (P("grp", "tp"), P(), P(None, "tp"), P())
    out_specs = P("grp", "tp")
    return jax.shard_map(
        on_device, mesh=mesh, in_specs=in_specs, out_specs=out_specs, check_vma=False
    )
```
